32 devices in a mesh: gx: 4 (over y, core), gy: 8 (over z, x).
Axes of the slice: x: 2, y: 2, z: 4, core: 2. Of those that a mesh axis runs over, the one named last changes fastest.
Arguments:
- tokens: bfloat16 [256, 4096], P('gy', 'gx'), may hold values from -140 to 140
- cotangent: bfloat16 [256, 4096], P('gy', 'gx'), may hold values from -6 to 6
- gate_weight: bfloat16 [4096, 14336], P('gx', 'gy'), may hold values from -5 to 5
- up_weight: bfloat16 [4096, 14336], P('gx', 'gy'), may hold values from -5 to 5
- down_weight: bfloat16 [14336, 4096], P('gy', 'gx'), may hold values from -5 to 5
Outputs:
- output: bfloat16 [256, 4096], P('gy', 'gx')
- input_grad: bfloat16 [256, 4096], P('gy', 'gx')
- gate_grad: bfloat16 [4096, 14336], P('gx', 'gy')
- up_grad: bfloat16 [4096, 14336], P('gx', 'gy')
- down_grad: bfloat16 [14336, 4096], P('gy', 'gx')
The draws below stay inside these ranges and needn't reach their ends.
All inputs are finite; a program needn't handle non-finite values.
Results may differ from the reference program's by a relative error of at most 0.005.
The reference program's roundings to bfloat16 on the way count: a program that leaves them out, or rounds other values in their place, can miss the bound.
Values may be sent and summed in bfloat16 or wider, within the bound.
A program may use at most 128 MiB of HBM per device.

```python
import jax
import jax.numpy as jnp
from jax import lax

D = 4096
FF = 14336
ROT_BLOCK = 128
HID_BLOCK = 64
TOKENS = 256


def rising_weight(key, row_total, col_total, fan_in):
    key_base, key_cols = jax.random.split(key)
    base = jnp.clip(jax.random.normal(key_base, (row_total, col_total), jnp.float32), -4.0, 4.0)
    row_frac = jnp.arange(row_total, dtype=jnp.float32)[:, None] / max(row_total - 1, 1)
    col_frac = jnp.arange(col_total, dtype=jnp.float32)[None, :] / max(col_total - 1, 1)
    col_rough = jnp.exp(jax.random.uniform(key_cols, (1, col_total), jnp.float32, 0.0, jnp.log(3.0)))
    rise = jnp.exp(jnp.log(3.0) * (row_frac + col_frac)) * col_rough
    return base * rise / (3.0 * fan_in ** 0.5)


def draw_tokens(key, part):
    key_base, key_rows, key_cols = jax.random.split(jax.random.fold_in(key, 11), 3)
    base = jnp.clip(jax.random.normal(key_base, (TOKENS, D), jnp.float32), -4.0, 4.0)
    row_rough = jnp.exp(jax.random.uniform(key_rows, (TOKENS, 1), jnp.float32, 0.0, jnp.log(3.3)))
    col_rough = jnp.exp(jax.random.uniform(key_cols, (1, D), jnp.float32, 0.0, jnp.log(3.0)))
    row_frac = jnp.arange(TOKENS, dtype=jnp.float32)[:, None] / max(TOKENS - 1, 1)
    col_frac = jnp.arange(D, dtype=jnp.float32)[None, :] / max(D - 1, 1)
    rise = jnp.exp(jnp.log(3.0) * (row_frac + col_frac))
    return (base * rise * row_rough * col_rough / 8.0).astype(jnp.bfloat16)


def draw_gate_weight(key, part):
    return rising_weight(jax.random.fold_in(key, 21), D, FF, D).astype(jnp.bfloat16)


def draw_up_weight(key, part):
    return rising_weight(jax.random.fold_in(key, 31), D, FF, D).astype(jnp.bfloat16)


def draw_down_weight(key, part):
    return rising_weight(jax.random.fold_in(key, 41), FF, D, FF).astype(jnp.bfloat16)


def block_levels(rng, extent, cuts, least, largest):
    loudness = 1.0
    for dim, parts in cuts:
        draws = jax.random.uniform(jax.random.fold_in(jax.random.fold_in(rng, 6), dim), (parts,), jnp.float32, least / len(cuts), largest / len(cuts))
        loudness = loudness * jnp.repeat(jnp.exp(draws), extent[dim] // parts).reshape((-1,) + (1,) * (len(extent) - 1 - dim))
    return loudness


def gaussian(own_key, shape, spread, most, cuts=(), kind=jnp.bfloat16):
    factor_of = block_levels(own_key, shape, cuts, -0.22, 0.18) if cuts else 1.0
    array = jax.random.normal(own_key, shape, jnp.float32) * spread * factor_of
    return jnp.minimum(jnp.maximum(array, -most), most).astype(kind)


def setup_inputs(seed: int = 0) -> dict:
    keys = jax.random.split(jax.random.key(seed), 6)
    return {
        "tokens": draw_tokens(jax.random.fold_in(keys[5], 71), 0),
        "cotangent": gaussian(keys[1], (TOKENS, D), 1.0, 6.0, ((0, 8), (1, 4))),
        "gate_weight": draw_gate_weight(jax.random.fold_in(keys[5], 71), 0),
        "up_weight": draw_up_weight(jax.random.fold_in(keys[5], 71), 0),
        "down_weight": draw_down_weight(jax.random.fold_in(keys[5], 71), 0),
    }


fp_top = 448.0
tiny = 1e-6


def hadamard_table(block_size):
    row_ids = jnp.arange(block_size, dtype=jnp.int32)[:, None]
    col_ids = jnp.arange(block_size, dtype=jnp.int32)[None, :]
    shared = row_ids & col_ids
    parity = jnp.zeros((block_size, block_size), jnp.int32)
    for bit_pos in range(max(block_size.bit_length() - 1, 1)):
        parity = parity + ((shared >> bit_pos) & 1)
    return (1 - 2 * (parity % 2)).astype(jnp.float32)


def rotate_cols(matrix, block_size):
    row_total, col_total = matrix.shape
    table = hadamard_table(block_size)
    blocks = matrix.astype(jnp.float32).reshape(row_total, col_total // block_size, block_size)
    turned = jnp.einsum("rbk,kl->rbl", blocks, table, precision=lax.Precision.HIGHEST)
    return turned.reshape(row_total, col_total) * (block_size ** -0.5)


def rotate_rows(matrix, block_size):
    row_total, col_total = matrix.shape
    table = hadamard_table(block_size)
    blocks = matrix.astype(jnp.float32).reshape(row_total // block_size, block_size, col_total)
    turned = jnp.einsum("kl,bkc->blc", table, blocks, precision=lax.Precision.HIGHEST)
    return turned.reshape(row_total, col_total) * (block_size ** -0.5)


def soft_cast(values, top):
    return (fp_top * jnp.tanh(values / (top + tiny))).astype(jnp.bfloat16)


def peak(values):
    return jnp.max(jnp.abs(values))


def reference(tokens, cotangent, gate_weight, up_weight, down_weight):
    token_rot = rotate_cols(tokens, ROT_BLOCK)
    gate_rot = rotate_rows(gate_weight, ROT_BLOCK)
    up_rot = rotate_rows(up_weight, ROT_BLOCK)
    down_rot = rotate_rows(down_weight, HID_BLOCK)
    token_peak = peak(token_rot)
    gate_peak = peak(gate_rot)
    up_peak = peak(up_rot)
    down_peak = peak(down_rot)
    token_cast = soft_cast(token_rot, token_peak)
    gate_cast = soft_cast(gate_rot, gate_peak)
    up_cast = soft_cast(up_rot, up_peak)
    down_cast = soft_cast(down_rot, down_peak)
    gate_pre = jnp.dot(token_cast, gate_cast, preferred_element_type=jnp.float32) * (token_peak * gate_peak / (fp_top * fp_top))
    up_pre = jnp.dot(token_cast, up_cast, preferred_element_type=jnp.float32) * (token_peak * up_peak / (fp_top * fp_top))
    hidden = (jax.nn.silu(gate_pre) * up_pre).astype(jnp.bfloat16)
    hidden_rot = rotate_cols(hidden, HID_BLOCK)
    hidden_peak = peak(hidden_rot)
    hidden_cast = soft_cast(hidden_rot, hidden_peak)
    output = (jnp.dot(hidden_cast, down_cast, preferred_element_type=jnp.float32) * (hidden_peak * down_peak / (fp_top * fp_top))).astype(jnp.bfloat16)
    down_grad = rotate_rows(jnp.dot(hidden_cast.T, cotangent, preferred_element_type=jnp.float32) * (hidden_peak / fp_top), HID_BLOCK).astype(jnp.bfloat16)
    hidden_grad = rotate_cols(jnp.dot(cotangent, down_cast.T, preferred_element_type=jnp.float32) * (down_peak / fp_top), HID_BLOCK)
    sigmoid_gate = jax.nn.sigmoid(gate_pre)
    gate_act = (hidden_grad * up_pre * sigmoid_gate * (1.0 + gate_pre * (1.0 - sigmoid_gate))).astype(jnp.bfloat16)
    up_act = (hidden_grad * gate_pre * sigmoid_gate).astype(jnp.bfloat16)
    gate_grad = rotate_rows(jnp.dot(token_cast.T, gate_act, preferred_element_type=jnp.float32) * (token_peak / fp_top), ROT_BLOCK).astype(jnp.bfloat16)
    up_grad = rotate_rows(jnp.dot(token_cast.T, up_act, preferred_element_type=jnp.float32) * (token_peak / fp_top), ROT_BLOCK).astype(jnp.bfloat16)
    input_sum = jnp.dot(gate_act, gate_cast.T, preferred_element_type=jnp.float32) * (gate_peak / fp_top) + jnp.dot(up_act, up_cast.T, preferred_element_type=jnp.float32) * (up_peak / fp_top)
    input_grad = rotate_cols(input_sum, ROT_BLOCK).astype(jnp.bfloat16)
    return (output, input_grad, gate_grad, up_grad, down_grad)
```

```python
import functools

import jax
import jax.numpy as jnp
from jax import lax
from jax.experimental import pallas as pl
from jax.experimental.pallas import tpu as pltpu
from jax.sharding import PartitionSpec as P

ROT_BLOCK = 128
HID_BLOCK = 64
CORES = 2

fp_top = 448.0
tiny = 1e-06

MESH = pl.DeviceIdType.MESH
VMEM = pl.BlockSpec(memory_space=pltpu.VMEM)
DMA = pltpu.SemaphoreType.DMA


def hadamard_table(block_size):
    row_ids = jnp.arange(block_size, dtype=jnp.int32)[:, None]
    col_ids = jnp.arange(block_size, dtype=jnp.int32)[None, :]
    shared = row_ids & col_ids
    parity = jnp.zeros((block_size, block_size), jnp.int32)
    for bit_pos in range(max(block_size.bit_length() - 1, 1)):
        parity = parity + (shared >> bit_pos & 1)
    return (1 - 2 * (parity % 2)).astype(jnp.float32)


def rotate_cols(matrix, block_size):
    row_total, col_total = matrix.shape
    table = hadamard_table(block_size)
    blocks = matrix.reshape(row_total, col_total // block_size, block_size)
    if matrix.dtype == jnp.bfloat16:
        turned = jnp.einsum(
            "rbk,kl->rbl", blocks, table.astype(jnp.bfloat16), preferred_element_type=jnp.float32
        )
    else:
        turned = jnp.einsum("rbk,kl->rbl", blocks, table, precision=lax.Precision.HIGHEST)
    return turned.reshape(row_total, col_total) * block_size ** (-0.5)


def rotate_rows(matrix, block_size):
    row_total, col_total = matrix.shape
    table = hadamard_table(block_size)
    blocks = matrix.reshape(row_total // block_size, block_size, col_total)
    turned = jnp.einsum(
        "kl,bkc->blc", table.astype(jnp.bfloat16), blocks, preferred_element_type=jnp.float32
    )
    return turned.reshape(row_total, col_total) * block_size ** (-0.5)


def soft_cast(values, top):
    return (fp_top * jnp.tanh(values / (top + tiny))).astype(jnp.bfloat16)


def peak(values):
    return jnp.max(jnp.abs(values))


def contract_rows(left_mat, right_mat):
    return lax.dot_general(
        left_mat, right_mat, (((0,), (0,)), ((), ())), preferred_element_type=jnp.float32
    )


def contract_cols(left_mat, right_mat):
    return lax.dot_general(
        left_mat, right_mat, (((1,), (1,)), ((), ())), preferred_element_type=jnp.float32
    )


def remote(src, dst, send, recv, target):
    return pltpu.make_async_remote_copy(
        src_ref=src, dst_ref=dst, send_sem=send, recv_sem=recv,
        device_id=target, device_id_type=MESH,
    )


def loop(low, high, body):
    def step(i, carry):
        body(i)
        return carry
    lax.fori_loop(low, high, step, 0)


def greet(n, me, axis):
    barrier = pltpu.get_barrier_semaphore()

    def hello(k):
        pl.semaphore_signal(
            barrier, inc=1, device_id={axis: lax.rem(me + k, n)}, device_id_type=MESH
        )

    loop(1, n, hello)


def exchange(n, me, axis, src, slots, send, recv):
    def copy(k, slot):
        return remote(
            src, slots.at[slot], send.at[k], recv.at[k], {axis: lax.rem(me + k, n)}
        )

    def start(k):
        copy(k, me).start()

    def finish(k):
        copy(k, lax.rem(me + n - k, n)).wait()

    return (lambda: loop(1, n, start)), (lambda: loop(1, n, finish))


def wide_gather_kernel(nx, ny, count, *refs):
    blocks, tile = refs[:count], refs[count]
    outs, tile_out = refs[count + 1 : 2 * count + 1], refs[2 * count + 1]
    slots_x, slots_y, mid, send, recv, sx, rx, sy, ry = refs[2 * count + 2 :]
    gx, gy = lax.axis_index("gx"), lax.axis_index("gy")
    greet(nx, gx, "gx")
    greet(ny, gy, "gy")
    pl.semaphore_wait(pltpu.get_barrier_semaphore(), nx - 1 + ny - 1)

    start_x, finish_x = exchange(nx, gx, "gx", tile, slots_x, sx, rx)
    start_y, finish_y = exchange(ny, gy, "gy", mid, slots_y, sy, ry)
    start_x()
    bulk = [
        exchange(ny, gy, "gy", blocks[i], outs[i], send.at[i], recv.at[i]) for i in range(count)
    ]
    slots_x[gx] = tile[...]
    for i in range(count):
        outs[i][gy] = blocks[i][...]
    finish_x()
    mid[...] = jnp.max(slots_x[...], axis=0)
    start_y()
    for begin, _ in bulk:
        begin()
    slots_y[gy] = mid[...]
    finish_y()
    tile_out[...] = jnp.max(slots_y[...], axis=0)
    for _, end in bulk:
        end()


def wide_gather(nx, ny, blocks, tile):
    count = len(blocks)
    return pl.pallas_call(
        functools.partial(wide_gather_kernel, nx, ny, count),
        out_shape=[jax.ShapeDtypeStruct((ny,) + b.shape, b.dtype) for b in blocks]
        + [jax.ShapeDtypeStruct(tile.shape, tile.dtype)],
        in_specs=[VMEM] * (count + 1),
        out_specs=[VMEM] * (count + 1),
        scratch_shapes=[
            pltpu.VMEM((nx,) + tile.shape, tile.dtype),
            pltpu.VMEM((ny,) + tile.shape, tile.dtype),
            pltpu.VMEM(tile.shape, tile.dtype),
            DMA((count, ny)), DMA((count, ny)),
            DMA((nx,)), DMA((nx,)), DMA((ny,)), DMA((ny,)),
        ],
        compiler_params=pltpu.CompilerParams(collective_id=0, has_side_effects=True),
    )(*blocks, tile)


def chip_scatter_kernel(nx, count, *refs):
    parts, outs = refs[:count], refs[count : 2 * count]
    first = refs[2 * count : 3 * count]
    second = refs[3 * count : 4 * count]
    third = refs[4 * count : 5 * count]
    s1, r1, s2, r2 = refs[5 * count :]
    gx = lax.axis_index("gx")
    y, core = gx // CORES, lax.rem(gx, CORES)
    other = 1 - core
    ys = nx // CORES
    greet(nx, gx, "gx")
    pl.semaphore_wait(pltpu.get_barrier_semaphore(), nx - 1)
    rows = outs[0].shape[0]
    step = 16

    def near(i, k):
        j = lax.rem(y + k, ys)
        return remote(
            parts[i].at[CORES * j + other], first[i].at[k], s1.at[i, k], r1.at[i, k],
            {"gx": CORES * y + other},
        )

    def far(i, k, slot):
        j = lax.rem(y + k, ys)
        return remote(
            second[i].at[k], third[i].at[slot], s2.at[i, k], r2.at[i, k],
            {"gx": CORES * j + core},
        )

    order = list(range(1, ys)) + [0]
    for k in order:
        for i in range(count):
            near(i, k).start()
    for k in order[:-1]:
        j = lax.rem(y + k, ys)
        for i in range(count):
            near(i, k).wait()

            def add(r, i=i, k=k, j=j):
                at = pl.ds(pl.multiple_of(r * step, step), step)
                total = parts[i][CORES * j + core, at, :] + first[i][k, at, :]
                second[i][k, at, :] = total.astype(jnp.bfloat16)

            loop(0, rows // step, add)
            far(i, k, k).start()
    for i in range(count):
        near(i, 0).wait()
    for i in range(count):
        for k in order[:-1]:
            far(i, k, k).wait()

        def close(r, i=i):
            at = pl.ds(pl.multiple_of(r * step, step), step)
            total = parts[i][CORES * y + core, at, :] + first[i][0, at, :]
            for k in order[:-1]:
                total = total + third[i][k, at, :].astype(jnp.float32)
            outs[i][at, :] = total

        loop(0, rows // step, close)


def chip_scatter(nx, parts):
    count, ys = len(parts), nx // CORES
    near = [pltpu.VMEM((ys,) + p.shape[1:], jnp.float32) for p in parts]
    far = [pltpu.VMEM((ys,) + p.shape[1:], jnp.bfloat16) for p in parts]
    return pl.pallas_call(
        functools.partial(chip_scatter_kernel, nx, count),
        out_shape=[jax.ShapeDtypeStruct(p.shape[1:], jnp.float32) for p in parts],
        in_specs=[VMEM] * count,
        out_specs=[VMEM] * count,
        scratch_shapes=near + far * 2
        + [DMA((count, ys)), DMA((count, ys)), DMA((count, ys)), DMA((count, ys))],
        compiler_params=pltpu.CompilerParams(collective_id=1, has_side_effects=True),
    )(*parts)


def chip_gather_kernel(nx, ny, count, *refs):
    blocks, tile = refs[:count], refs[count]
    outs, tile_out = refs[count + 1 : 2 * count + 1], refs[2 * count + 1]
    slots_x, slots_y, mid, sn, rn, sf, rf, sx, rx, sy, ry = refs[2 * count + 2 :]
    gx, gy = lax.axis_index("gx"), lax.axis_index("gy")
    y, core = gx // CORES, lax.rem(gx, CORES)
    other = 1 - core
    ys = nx // CORES
    greet(nx, gx, "gx")
    greet(ny, gy, "gy")
    pl.semaphore_wait(pltpu.get_barrier_semaphore(), nx - 1 + ny - 1)

    start_x, finish_x = exchange(nx, gx, "gx", tile, slots_x, sx, rx)
    start_y, finish_y = exchange(ny, gy, "gy", mid, slots_y, sy, ry)
    start_x()

    def far(i, k, slot):
        j = lax.rem(y + k, ys)
        return remote(
            blocks[i], outs[i].at[slot], sf.at[i, k], rf.at[i, k], {"gx": CORES * j + core}
        )

    def near(i, k, src, slot):
        return remote(
            src, outs[i].at[slot], sn.at[i, k], rn.at[i, k], {"gx": CORES * y + other}
        )

    for k in range(1, ys):
        for i in range(count):
            far(i, k, gx).start()
    for i in range(count):
        near(i, 0, blocks[i], gx).start()
    slots_x[gx] = tile[...]
    for i in range(count):
        outs[i][gx] = blocks[i][...]
    finish_x()
    mid[...] = jnp.max(slots_x[...], axis=0)
    start_y()
    slots_y[gy] = mid[...]
    finish_y()
    tile_out[...] = jnp.max(slots_y[...], axis=0)
    for k in range(1, ys):
        j = lax.rem(y + ys - k, ys)
        mine = CORES * j + core
        for i in range(count):
            far(i, k, mine).wait()
            near(i, k, outs[i].at[mine], mine).start()
    for i in range(count):
        near(i, 0, blocks[i], CORES * y + other).wait()
        for k in range(1, ys):
            j = lax.rem(y + ys - k, ys)
            near(i, k, outs[i].at[CORES * j + core], CORES * j + other).wait()


def chip_gather(nx, ny, blocks, tile):
    count, ys = len(blocks), nx // CORES
    return pl.pallas_call(
        functools.partial(chip_gather_kernel, nx, ny, count),
        out_shape=[jax.ShapeDtypeStruct((nx,) + b.shape, b.dtype) for b in blocks]
        + [jax.ShapeDtypeStruct(tile.shape, tile.dtype)],
        in_specs=[VMEM] * (count + 1),
        out_specs=[VMEM] * (count + 1),
        scratch_shapes=[
            pltpu.VMEM((nx,) + tile.shape, tile.dtype),
            pltpu.VMEM((ny,) + tile.shape, tile.dtype),
            pltpu.VMEM(tile.shape, tile.dtype),
            DMA((count, ys)), DMA((count, ys)), DMA((count, ys)), DMA((count, ys)),
            DMA((nx,)), DMA((nx,)), DMA((ny,)), DMA((ny,)),
        ],
        compiler_params=pltpu.CompilerParams(collective_id=2, has_side_effects=True),
    )(*blocks, tile)


def wide_scatter_kernel(ny, count, *refs):
    parts, outs = refs[:count], refs[count : 2 * count]
    slots = refs[2 * count : 3 * count]
    send, recv = refs[3 * count :]
    gy = lax.axis_index("gy")
    greet(ny, gy, "gy")
    pl.semaphore_wait(pltpu.get_barrier_semaphore(), ny - 1)

    def copy(i, k):
        j = lax.rem(gy + k, ny)
        return remote(
            parts[i].at[j], slots[i].at[k], send.at[i, k], recv.at[i, k], {"gy": j}
        )

    for i in range(count):
        loop(1, ny, lambda k, i=i: copy(i, k).start())
    for i in range(count):
        outs[i][...] = parts[i][gy].astype(jnp.float32)

        def add(k, i=i):
            copy(i, k).wait()
            outs[i][...] += slots[i][k].astype(jnp.float32)

        loop(1, ny, add)


def wide_scatter(ny, parts):
    count = len(parts)
    return pl.pallas_call(
        functools.partial(wide_scatter_kernel, ny, count),
        out_shape=[jax.ShapeDtypeStruct(p.shape[1:], jnp.float32) for p in parts],
        in_specs=[VMEM] * count,
        out_specs=[VMEM] * count,
        scratch_shapes=[pltpu.VMEM(p.shape, p.dtype) for p in parts]
        + [DMA((count, ny)), DMA((count, ny))],
        compiler_params=pltpu.CompilerParams(collective_id=3, has_side_effects=True),
    )(*parts)


def peak_tile(values):
    column = jnp.stack(values + [values[0]] * (8 - len(values)))[:, None]
    return jnp.broadcast_to(column, (8, 128))


def shards(nx, ny, tokens, cotangent, gate_weight, up_weight, down_weight):
    gate_rot = rotate_rows(gate_weight, ROT_BLOCK)
    up_rot = rotate_rows(up_weight, ROT_BLOCK)
    down_rot = rotate_rows(down_weight, HID_BLOCK)
    own_peaks = [
        peak(rotate_cols(tokens, ROT_BLOCK)), peak(gate_rot), peak(up_rot), peak(down_rot)
    ]
    all_tokens, all_cot, peaks = wide_gather(nx, ny, [tokens, cotangent], peak_tile(own_peaks))
    token_peak, gate_peak, up_peak, down_peak = (peaks[i, 0] for i in range(4))
    width = tokens.shape[1]
    all_tokens = all_tokens.reshape(-1, width)
    all_cot = all_cot.reshape(-1, width)
    token_total = all_tokens.shape[0]
    gate_cast = soft_cast(gate_rot, gate_peak)
    up_cast = soft_cast(up_rot, up_peak)
    down_cast = soft_cast(down_rot, down_peak)
    hid_width = gate_weight.shape[1]
    token_cast = soft_cast(rotate_cols(all_tokens, ROT_BLOCK), token_peak)

    def split(matrix, n):
        return matrix.reshape(n, token_total // n, matrix.shape[1])

    gate_sum, up_sum, back_sum = chip_scatter(
        nx,
        [
            split(jnp.dot(token_cast, gate_cast, preferred_element_type=jnp.float32), nx),
            split(jnp.dot(token_cast, up_cast, preferred_element_type=jnp.float32), nx),
            split(contract_cols(all_cot, down_cast), nx),
        ],
    )
    gate_pre = gate_sum * (token_peak * gate_peak / (fp_top * fp_top))
    up_pre = up_sum * (token_peak * up_peak / (fp_top * fp_top))
    sigmoid_gate = jax.nn.sigmoid(gate_pre)
    hidden = (gate_pre * sigmoid_gate * up_pre).astype(jnp.bfloat16)
    own_peak = peak(rotate_cols(hidden, HID_BLOCK))
    hidden_grad = rotate_cols(back_sum * (down_peak / fp_top), HID_BLOCK)
    gate_act = (
        hidden_grad * up_pre * sigmoid_gate * (1.0 + gate_pre * (1.0 - sigmoid_gate))
    ).astype(jnp.bfloat16)
    up_act = (hidden_grad * gate_pre * sigmoid_gate).astype(jnp.bfloat16)
    all_hidden, all_gate_act, all_up_act, tops = chip_gather(
        nx, ny, [hidden, gate_act, up_act], peak_tile([own_peak])
    )
    hidden_peak = tops[0, 0]
    all_hidden = all_hidden.reshape(-1, hid_width)
    all_gate_act = all_gate_act.reshape(-1, hid_width)
    all_up_act = all_up_act.reshape(-1, hid_width)
    hidden_cast = soft_cast(rotate_cols(all_hidden, HID_BLOCK), hidden_peak)
    out_part = jnp.dot(hidden_cast, down_cast, preferred_element_type=jnp.float32)
    input_part = contract_cols(all_gate_act, gate_cast) * (gate_peak / fp_top) + contract_cols(
        all_up_act, up_cast
    ) * (up_peak / fp_top)
    out_sum, input_sum = wide_scatter(
        ny, [split(part.astype(jnp.bfloat16), ny) for part in (out_part, input_part)]
    )
    output = (out_sum * (hidden_peak * down_peak / (fp_top * fp_top))).astype(jnp.bfloat16)
    input_grad = rotate_cols(input_sum, ROT_BLOCK).astype(jnp.bfloat16)
    hidden_turned = rotate_cols(hidden_cast, HID_BLOCK).astype(jnp.bfloat16)
    token_turned = rotate_cols(token_cast, ROT_BLOCK).astype(jnp.bfloat16)
    down_grad = (contract_rows(hidden_turned, all_cot) * (hidden_peak / fp_top)).astype(
        jnp.bfloat16
    )
    gate_grad = (contract_rows(token_turned, all_gate_act) * (token_peak / fp_top)).astype(
        jnp.bfloat16
    )
    up_grad = (contract_rows(token_turned, all_up_act) * (token_peak / fp_top)).astype(jnp.bfloat16)
    return (output, input_grad, gate_grad, up_grad, down_grad)


def solution(mesh):
    in_specs = (P("gy", "gx"), P("gy", "gx"), P("gx", "gy"), P("gx", "gy"), P("gy", "gx"))
    out_specs = (P("gy", "gx"), P("gy", "gx"), P("gx", "gy"), P("gx", "gy"), P("gy", "gx"))
    nx, ny = mesh.shape["gx"], mesh.shape["gy"]
    return jax.shard_map(
        functools.partial(shards, nx, ny),
        mesh=mesh, in_specs=in_specs, out_specs=out_specs, check_vma=False,
    )
```

```python
import functools

import jax
import jax.numpy as jnp
from jax import lax
from jax.experimental import pallas as pl
from jax.experimental.pallas import tpu as pltpu
from jax.sharding import PartitionSpec as P

ROT_BLOCK = 128
HID_BLOCK = 64
CORES = 2

fp_top = 448.0
tiny = 1e-06

MESH = pl.DeviceIdType.MESH
VMEM = pl.BlockSpec(memory_space=pltpu.VMEM)
DMA = pltpu.SemaphoreType.DMA


def hadamard_table(block_size):
    row_ids = jnp.arange(block_size, dtype=jnp.int32)[:, None]
    col_ids = jnp.arange(block_size, dtype=jnp.int32)[None, :]
    shared = row_ids & col_ids
    parity = jnp.zeros((block_size, block_size), jnp.int32)
    for bit_pos in range(max(block_size.bit_length() - 1, 1)):
        parity = parity + (shared >> bit_pos & 1)
    return (1 - 2 * (parity % 2)).astype(jnp.float32)


def rotate_cols(matrix, block_size):
    row_total, col_total = matrix.shape
    table = hadamard_table(block_size)
    blocks = matrix.reshape(row_total, col_total // block_size, block_size)
    if matrix.dtype == jnp.bfloat16:
        turned = jnp.einsum(
            "rbk,kl->rbl", blocks, table.astype(jnp.bfloat16), preferred_element_type=jnp.float32
        )
    else:
        turned = jnp.einsum("rbk,kl->rbl", blocks, table, precision=lax.Precision.HIGHEST)
    return turned.reshape(row_total, col_total) * block_size ** (-0.5)


def rotate_rows(matrix, block_size):
    row_total, col_total = matrix.shape
    table = hadamard_table(block_size)
    blocks = matrix.reshape(row_total // block_size, block_size, col_total)
    turned = jnp.einsum(
        "kl,bkc->blc", table.astype(jnp.bfloat16), blocks, preferred_element_type=jnp.float32
    )
    return turned.reshape(row_total, col_total) * block_size ** (-0.5)


def soft_cast(values, top):
    return (fp_top * jnp.tanh(values / top)).astype(jnp.bfloat16)


def peak(values):
    return jnp.max(jnp.abs(values))


def contract_rows(left_mat, right_mat):
    return lax.dot_general(
        left_mat, right_mat, (((0,), (0,)), ((), ())), preferred_element_type=jnp.float32
    )


def contract_cols(left_mat, right_mat):
    return lax.dot_general(
        left_mat, right_mat, (((1,), (1,)), ((), ())), preferred_element_type=jnp.float32
    )


def remote(src, dst, send, recv, target):
    return pltpu.make_async_remote_copy(
        src_ref=src, dst_ref=dst, send_sem=send, recv_sem=recv,
        device_id=target, device_id_type=MESH,
    )


def loop(low, high, body):
    def step(i, carry):
        body(i)
        return carry
    lax.fori_loop(low, high, step, 0)


def greet(n, me, axis):
    barrier = pltpu.get_barrier_semaphore()

    def hello(k):
        pl.semaphore_signal(
            barrier, inc=1, device_id={axis: lax.rem(me + k, n)}, device_id_type=MESH
        )

    loop(1, n, hello)


def exchange(n, me, axis, src, slots, send, recv):
    def copy(k, slot):
        return remote(
            src, slots.at[slot], send.at[k], recv.at[k], {axis: lax.rem(me + k, n)}
        )

    def start(k):
        copy(k, me).start()

    def finish(k):
        copy(k, lax.rem(me + n - k, n)).wait()

    return (lambda: loop(1, n, start)), (lambda: loop(1, n, finish))


def scatter_kernel(axis, n, inner, count, *refs):
    parts, outs = refs[:count], refs[count : 2 * count]
    first = refs[2 * count : 3 * count]
    second = refs[3 * count : 4 * count]
    third = refs[4 * count : 5 * count]
    s1, r1, s2, r2 = refs[5 * count :]
    me = lax.axis_index(axis)
    hi, lo = me // inner, lax.rem(me, inner)
    outer = n // inner
    greet(n, me, axis)
    pl.semaphore_wait(pltpu.get_barrier_semaphore(), n - 1)
    rows = outs[0].shape[0]
    step = 16

    def near(i, k, o):
        j, to = lax.rem(hi + k, outer), lax.rem(lo + o, inner)
        return remote(
            parts[i].at[inner * j + to], first[i].at[k * inner + o], s1.at[i, k, o],
            r1.at[i, k, o], {axis: inner * hi + to},
        )

    def far(i, k):
        j = lax.rem(hi + k, outer)
        return remote(
            second[i].at[k], third[i].at[k], s2.at[i, k], r2.at[i, k], {axis: inner * j + lo}
        )

    def inner_sum(i, k, at):
        total = parts[i][inner * lax.rem(hi + k, outer) + lo, at, :].astype(jnp.float32)
        for o in range(1, inner):
            total = total + first[i][k * inner + o, at, :].astype(jnp.float32)
        return total

    order = list(range(1, outer)) + [0]
    for k in order:
        for i in range(count):
            for o in range(1, inner):
                near(i, k, o).start()
    for k in order[:-1]:
        for i in range(count):
            for o in range(1, inner):
                near(i, k, o).wait()

            def add(r, i=i, k=k):
                at = pl.ds(pl.multiple_of(r * step, step), step)
                second[i][k, at, :] = inner_sum(i, k, at).astype(jnp.bfloat16)

            loop(0, rows // step, add)
            far(i, k).start()
    for i in range(count):
        for o in range(1, inner):
            near(i, 0, o).wait()
    for i in range(count):
        for k in order[:-1]:
            far(i, k).wait()

        def close(r, i=i):
            at = pl.ds(pl.multiple_of(r * step, step), step)
            total = inner_sum(i, 0, at)
            for k in order[:-1]:
                total = total + third[i][k, at, :].astype(jnp.float32)
            outs[i][at, :] = total

        loop(0, rows // step, close)


def scatter(axis, n, inner, parts, number):
    count, outer = len(parts), n // inner
    near = [pltpu.VMEM((n,) + p.shape[1:], p.dtype) for p in parts]
    far = [pltpu.VMEM((outer,) + p.shape[1:], jnp.bfloat16) for p in parts]
    return pl.pallas_call(
        functools.partial(scatter_kernel, axis, n, inner, count),
        out_shape=[jax.ShapeDtypeStruct(p.shape[1:], jnp.float32) for p in parts],
        in_specs=[VMEM] * count,
        out_specs=[VMEM] * count,
        scratch_shapes=near + far * 2
        + [DMA((count, outer, inner))] * 2 + [DMA((count, outer))] * 2,
        compiler_params=pltpu.CompilerParams(collective_id=number, has_side_effects=True),
    )(*parts)


def gather_kernel(axis, n, inner, nx, ny, count, *refs):
    blocks, tile = refs[:count], refs[count]
    outs, tile_out = refs[count + 1 : 2 * count + 1], refs[2 * count + 1]
    slots_x, slots_y, mid, sn, rn, sf, rf, sx, rx, sy, ry = refs[2 * count + 2 :]
    gx, gy = lax.axis_index("gx"), lax.axis_index("gy")
    me = lax.axis_index(axis)
    hi, lo = me // inner, lax.rem(me, inner)
    outer = n // inner
    greet(nx, gx, "gx")
    greet(ny, gy, "gy")
    pl.semaphore_wait(pltpu.get_barrier_semaphore(), nx - 1 + ny - 1)

    start_x, finish_x = exchange(nx, gx, "gx", tile, slots_x, sx, rx)
    start_y, finish_y = exchange(ny, gy, "gy", mid, slots_y, sy, ry)
    start_x()

    def far(i, k, slot):
        j = lax.rem(hi + k, outer)
        return remote(
            blocks[i], outs[i].at[slot], sf.at[i, k], rf.at[i, k], {axis: inner * j + lo}
        )

    def near(i, k, o, src, slot):
        return remote(
            src, outs[i].at[slot], sn.at[i, k, o], rn.at[i, k, o],
            {axis: inner * hi + lax.rem(lo + o, inner)},
        )

    for k in range(1, outer):
        for i in range(count):
            far(i, k, me).start()
    for i in range(count):
        for o in range(1, inner):
            near(i, 0, o, blocks[i], me).start()
    slots_x[gx] = tile[...]
    for i in range(count):
        outs[i][me] = blocks[i][...]
    finish_x()
    mid[...] = jnp.max(slots_x[...], axis=0)
    start_y()
    slots_y[gy] = mid[...]
    for k in range(1, outer):
        mine = inner * lax.rem(hi + outer - k, outer) + lo
        for i in range(count):
            far(i, k, mine).wait()
            for o in range(1, inner):
                near(i, k, o, outs[i].at[mine], mine).start()
    finish_y()
    top = jnp.max(slots_y[...], axis=0)
    tile_out[0] = top
    tile_out[1] = top + tiny
    tile_out[2] = top / fp_top
    tile_out[3] = top * top[0:1, :] / (fp_top * fp_top)
    for i in range(count):
        for o in range(1, inner):
            side = lax.rem(lo + inner - o, inner)
            near(i, 0, o, blocks[i], inner * hi + side).wait()
            for k in range(1, outer):
                row = inner * lax.rem(hi + outer - k, outer)
                near(i, k, o, outs[i].at[row + lo], row + side).wait()


def gather(axis, n, inner, nx, ny, blocks, tile, number):
    count, outer = len(blocks), n // inner
    return pl.pallas_call(
        functools.partial(gather_kernel, axis, n, inner, nx, ny, count),
        out_shape=[jax.ShapeDtypeStruct((n,) + b.shape, b.dtype) for b in blocks]
        + [jax.ShapeDtypeStruct((4,) + tile.shape, tile.dtype)],
        in_specs=[VMEM] * (count + 1),
        out_specs=[VMEM] * (count + 1),
        scratch_shapes=[
            pltpu.VMEM((nx,) + tile.shape, tile.dtype),
            pltpu.VMEM((ny,) + tile.shape, tile.dtype),
            pltpu.VMEM(tile.shape, tile.dtype),
        ]
        + [DMA((count, outer, inner))] * 2 + [DMA((count, outer))] * 2
        + [DMA((nx,))] * 2 + [DMA((ny,))] * 2,
        compiler_params=pltpu.CompilerParams(collective_id=number, has_side_effects=True),
    )(*blocks, tile)


def peak_tile(values):
    rows = lax.broadcasted_iota(jnp.int32, (8, 128), 0)
    tile = jnp.full((8, 128), values[0])
    for i, value in enumerate(values[1:], 1):
        tile = jnp.where(rows == i, value, tile)
    return tile


def shards(nx, ny, tokens, cotangent, gate_weight, up_weight, down_weight):
    lanes = 1 << ((ny.bit_length() - 2) // 2)
    gate_rot = rotate_rows(gate_weight, ROT_BLOCK)
    up_rot = rotate_rows(up_weight, ROT_BLOCK)
    down_rot = rotate_rows(down_weight, HID_BLOCK)
    own_peaks = [
        peak(rotate_cols(tokens, ROT_BLOCK)), peak(gate_rot), peak(up_rot), peak(down_rot)
    ]
    all_tokens, all_cot, peaks = gather(
        "gy", ny, lanes, nx, ny, [tokens, cotangent], peak_tile(own_peaks), 0
    )
    down_peak = peaks[0, 3, 0]
    token_top, gate_top, up_top, down_top = (peaks[1, i, 0] for i in range(4))
    token_unit, gate_unit, up_unit, down_unit = (peaks[2, i, 0] for i in range(4))
    width = tokens.shape[1]
    all_tokens = all_tokens.reshape(-1, width)
    all_cot = all_cot.reshape(-1, width)
    token_total = all_tokens.shape[0]
    gate_cast = soft_cast(gate_rot, gate_top)
    up_cast = soft_cast(up_rot, up_top)
    down_cast = soft_cast(down_rot, down_top)
    hid_width = gate_weight.shape[1]
    token_cast = soft_cast(rotate_cols(all_tokens, ROT_BLOCK), token_top)

    def split(matrix, n):
        return matrix.reshape(n, token_total // n, matrix.shape[1])

    gate_sum, up_sum, back_sum = scatter(
        "gx", nx, CORES,
        [
            split(jnp.dot(token_cast, gate_cast, preferred_element_type=jnp.float32), nx),
            split(jnp.dot(token_cast, up_cast, preferred_element_type=jnp.float32), nx),
            split(contract_cols(all_cot, down_cast), nx),
        ],
        1,
    )
    gate_pre = gate_sum * peaks[3, 1, 0]
    up_pre = up_sum * peaks[3, 2, 0]
    sigmoid_gate = jax.nn.sigmoid(gate_pre)
    hidden = (gate_pre * sigmoid_gate * up_pre).astype(jnp.bfloat16)
    own_peak = peak(rotate_cols(hidden, HID_BLOCK))
    hidden_grad = rotate_cols(back_sum * down_unit, HID_BLOCK)
    gate_act = (
        hidden_grad * up_pre * sigmoid_gate * (1.0 + gate_pre * (1.0 - sigmoid_gate))
    ).astype(jnp.bfloat16)
    up_act = (hidden_grad * gate_pre * sigmoid_gate).astype(jnp.bfloat16)
    all_hidden, all_gate_act, all_up_act, tops = gather(
        "gx", nx, CORES, nx, ny, [hidden, gate_act, up_act], peak_tile([own_peak, down_peak]), 2
    )
    hidden_top, hidden_unit = tops[1, 0, 0], tops[2, 0, 0]
    all_hidden = all_hidden.reshape(-1, hid_width)
    all_gate_act = all_gate_act.reshape(-1, hid_width)
    all_up_act = all_up_act.reshape(-1, hid_width)
    hidden_cast = soft_cast(rotate_cols(all_hidden, HID_BLOCK), hidden_top)
    out_part = jnp.dot(hidden_cast, down_cast, preferred_element_type=jnp.float32)
    input_part = contract_cols(all_gate_act, gate_cast) * gate_unit + contract_cols(
        all_up_act, up_cast
    ) * up_unit
    out_sum, input_sum = scatter(
        "gy", ny, lanes,
        [split(part.astype(jnp.bfloat16), ny) for part in (out_part, input_part)],
        3,
    )
    output = (out_sum * tops[3, 1, 0]).astype(jnp.bfloat16)
    input_grad = rotate_cols(input_sum, ROT_BLOCK).astype(jnp.bfloat16)
    hidden_turned = rotate_cols(hidden_cast, HID_BLOCK).astype(jnp.bfloat16)
    token_turned = rotate_cols(token_cast, ROT_BLOCK).astype(jnp.bfloat16)
    down_grad = (contract_rows(hidden_turned, all_cot) * hidden_unit).astype(
        jnp.bfloat16
    )
    gate_grad = (contract_rows(token_turned, all_gate_act) * token_unit).astype(
        jnp.bfloat16
    )
    up_grad = (contract_rows(token_turned, all_up_act) * token_unit).astype(jnp.bfloat16)
    return (output, input_grad, gate_grad, up_grad, down_grad)


def solution(mesh):
    in_specs = (P("gy", "gx"), P("gy", "gx"), P("gx", "gy"), P("gx", "gy"), P("gy", "gx"))
    out_specs = (P("gy", "gx"), P("gy", "gx"), P("gx", "gy"), P("gx", "gy"), P("gy", "gx"))
    nx, ny = mesh.shape["gx"], mesh.shape["gy"]
    return jax.shard_map(
        functools.partial(shards, nx, ny),
        mesh=mesh, in_specs=in_specs, out_specs=out_specs, check_vma=False,
    )
```
